32 devices in a mesh: ep: 2 (over y), tp: 16 (over z, x, core).
Axes of the slice: x: 2, y: 2, z: 4, core: 2. Of those that a mesh axis runs over, the one named last changes fastest.
Arguments:
- activations: bfloat16 [64, 6144], P(None, 'tp'), may hold values from -6 to 6
- norm_gain: float32 [6144], replicated, may hold values from 0.1 to 1.9
- router_weight: bfloat16 [6144, 8], P('tp'), may hold values from -0.078125 to 0.078125
- expert_ids: int32 [64, 2], replicated, may hold values from 0 to 7, all different within a row
- w_gate: bfloat16 [8, 6144, 2048], P('ep', None, 'tp'), may hold values from -0.078125 to 0.078125
- w_up: bfloat16 [8, 6144, 2048], P('ep', None, 'tp'), may hold values from -0.078125 to 0.078125
- w_down: bfloat16 [8, 2048, 6144], P('ep', 'tp'), may hold values from -0.1875 to 0.1875
Outputs:
- moe_out: bfloat16 [64, 6144], P(None, 'tp')
The draws below stay inside these ranges and needn't reach their ends.
Inputs may be any that keep to these rules, and one draw needn't show every extreme that they name: `expert_ids`: each row names two different experts from 0 to 7, and every expert is named by some token.
All inputs are finite; a program needn't handle non-finite values.
Results may differ from the reference program's by a relative error of at most 0.0025.
Values may be sent and summed in bfloat16 or wider, within the bound.
A program may use at most 64 MiB of HBM per device.

```python
import jax
import jax.numpy as jnp
from jax import lax

D = 6144
TOKENS = 64
EXPERTS = 8
FF = 2048


def raised(array, key, source, target, shards_of, factor):
    def block_of(position):
        return (jnp.arange(array.shape[position]) // (array.shape[position] // shards_of)).reshape((-1,) + (1,) * (array.ndim - 1 - position))

    one_side = jax.random.permutation(key, shards_of)[block_of(target)]
    other_side = (block_of(target) + shards_of // 2) % shards_of
    return jnp.where((block_of(source) == one_side) | (block_of(source) == other_side), factor * array, array)


def level_of(own_key, dims, pieces, low, top_value):
    def one(dim, blocks):
        draws = jax.random.uniform(jax.random.fold_in(jax.random.fold_in(own_key, 6), dim), (blocks,), jnp.float32, low / len(pieces), top_value / len(pieces))
        return jnp.repeat(jnp.exp(draws), dims[dim] // blocks).reshape((-1,) + (1,) * (len(dims) - dim - 1))

    factor_of = one(*pieces[0])
    for cut in pieces[1:]:
        factor_of = factor_of * one(*cut)
    return factor_of


def picks_of(stream_key, rows, number_of, top, lift):
    order = jax.random.permutation(jax.random.fold_in(stream_key, 1), number_of)
    boost = order
    for power in range(3):
        boost = boost * boost // number_of
    boost = boost * lift // number_of
    lots = jax.random.randint(jax.random.fold_in(stream_key, 2), (rows, number_of), 0, 4096) + boost
    sure = jax.random.permutation(jax.random.fold_in(stream_key, 3), rows)[jnp.arange(number_of) % rows]
    lots = jnp.where(jnp.arange(rows)[:, None] == sure[None, :], 1 << 14, lots)
    score = lots * number_of + jnp.arange(number_of)
    return lax.top_k(score.astype(jnp.int32), top)[1].astype(jnp.int32)


def bell_draw(stream_key, shape, deviation, most, cuts=(), kind=jnp.bfloat16):
    loudness = level_of(stream_key, shape, cuts, -0.22, 0.18) if cuts else 1.0
    values = jax.random.normal(stream_key, shape, jnp.float32) * deviation * loudness
    return jnp.minimum(jnp.maximum(values, -most), most).astype(kind)


def gaussian_with(own_key, extent, deviation, most, split, heavy, held_as=jnp.bfloat16):
    array = deviation * jax.random.normal(own_key, extent, jnp.float32)
    if split:
        array = array * level_of(own_key, extent, split, -0.22, 0.18)
    return jnp.clip(raised(array, jax.random.fold_in(own_key, 3), *heavy), -most, most).astype(held_as)


def setup_inputs(seed: int = 0) -> dict:
    keys = jax.random.split(jax.random.key(seed), 8)
    activations = bell_draw(keys[0], (TOKENS, D), 1.0, 6.0, ((1, 16),))
    norm_gain = jnp.clip(1.0 + 0.18 * jax.random.normal(keys[1], (D,), jnp.float32), 0.1, 1.9)
    router_weight = bell_draw(keys[2], (D, EXPERTS), D ** -0.5, 0.078125, ((0, 16),))
    expert_ids = picks_of(keys[3], TOKENS, EXPERTS, 2, 2048)
    w_gate = bell_draw(keys[4], (EXPERTS, D, FF), D ** -0.5, 0.078125, ((0, 2), (2, 16)))
    w_up = bell_draw(keys[5], (EXPERTS, D, FF), D ** -0.5, 0.078125, ((0, 2), (2, 16)))
    w_down = gaussian_with(keys[6], (EXPERTS, FF, D), FF ** -0.5, 0.1875, ((0, 2), (1, 16)), (1, 2, 16, 2.0))
    return dict(activations=activations, norm_gain=norm_gain, router_weight=router_weight, expert_ids=expert_ids, w_gate=w_gate, w_up=w_up, w_down=w_down)


epsilon = 1e-05

def reference(activations, norm_gain, router_weight, expert_ids, w_gate, w_up, w_down):
    features = activations.astype(jnp.float32)
    inv_rms = lax.rsqrt(lax.optimization_barrier(jnp.mean(features * features, axis=1, keepdims=True)) + epsilon)
    normed = (features * inv_rms * norm_gain.astype(jnp.float32)).astype(jnp.bfloat16)
    logits = jnp.dot(normed, router_weight, preferred_element_type=jnp.float32)
    chosen = jnp.take_along_axis(logits, expert_ids, axis=1)
    weights = jax.nn.softmax(chosen, axis=1)
    gate_dense = lax.optimization_barrier(jnp.sum(weights[:, :, None] * jax.nn.one_hot(expert_ids, EXPERTS, dtype=jnp.float32), axis=1))
    combined = jnp.zeros((TOKENS, D), jnp.float32)
    for expert in range(EXPERTS):
        gate_act = jnp.dot(normed, w_gate[expert], preferred_element_type=jnp.float32)
        up_act = jnp.dot(normed, w_up[expert], preferred_element_type=jnp.float32)
        hidden = (jax.nn.silu(gate_act) * up_act).astype(jnp.bfloat16)
        expert_out = jnp.dot(hidden, w_down[expert], preferred_element_type=jnp.float32)
        combined = combined + gate_dense[:, expert:expert + 1] * expert_out
    return combined.astype(jnp.bfloat16)
```

```python
import functools

import jax
import jax.numpy as jnp
from jax import lax
from jax.experimental import pallas as pl
from jax.experimental.pallas import tpu as pltpu
from jax.sharding import PartitionSpec as P

epsilon = 1e-05
MESH = pl.DeviceIdType.MESH


def layer_kernel(
    lines, local_count, x_hbm, gain_hbm, r_hbm, ids_hbm, wg_hbm, wu_hbm, wd_hbm, o_ref,
    x_all, r_all, gain, ids, wgu, wd, normed, rwide,
    pair_out, pair_in, own, ep_out, ep_in, side_out, side_in, line_out, line_in, last_out, last_in,
    load_sem, gu_sem, down_sem,
    z_send, z_recv, s_send, s_recv, c_send, c_recv,
    pair_ss, pair_rs, ep_ss, ep_rs, side_ss, side_rs, line_ss, line_rs, last_ss, last_rs,
):
    rows, width = x_all.shape[1], x_all.shape[2]
    half = rows // 2
    y = lax.axis_index("ep")
    t = lax.axis_index("tp")
    c = t % 2
    x = (t // 2) % 2
    z = t // 4

    def index(zz, xx, cc):
        return (zz * 2 + xx) * 2 + cc

    def at_z(step):
        return (z + step) % lines

    pair = (y, index(z, x, 1 - c))
    side = (y, index(z, 1 - x, c))
    other = (1 - y, t)

    def along(step):
        return (y, index(at_z(step), x, c))

    loads = [
        pltpu.make_async_copy(x_hbm, x_all.at[t], load_sem.at[0]),
        pltpu.make_async_copy(r_hbm, r_all.at[t], load_sem.at[1]),
        pltpu.make_async_copy(gain_hbm, gain, load_sem.at[2]),
        pltpu.make_async_copy(ids_hbm, ids, load_sem.at[3]),
    ]
    for load in loads:
        load.start()
    inner = wg_hbm.shape[2]
    gu_loads = []
    for e in range(local_count):
        gu_loads.append(pltpu.make_async_copy(wg_hbm.at[e], wgu.at[e, :, pl.ds(0, inner)], gu_sem.at[e, 0]))
        gu_loads.append(pltpu.make_async_copy(wu_hbm.at[e], wgu.at[e, :, pl.ds(inner, inner)], gu_sem.at[e, 1]))
    for load in gu_loads:
        load.start()
    down_load = pltpu.make_async_copy(wd_hbm, wd, down_sem.at[0])
    down_load.start()

    barrier = pltpu.get_barrier_semaphore()
    peers = [pair, side, other] + [along(step) for step in range(1, lines)]
    for peer in peers:
        pl.semaphore_signal(barrier, inc=1, device_id=peer, device_id_type=MESH)
    pl.semaphore_wait(barrier, len(peers))

    def remote(src, dst, ss, rs, peer):
        return pltpu.make_async_remote_copy(
            src_ref=src, dst_ref=dst, send_sem=ss, recv_sem=rs, device_id=peer, device_id_type=MESH
        )

    sent = []

    def gather(buf, kind):
        def block(i):
            return buf.at[i]

        zs, ss, cs = [], [], []
        for step in range(1, lines):
            zs.append(remote(block(t), block(t), z_send.at[kind, step], z_recv.at[kind, step], along(step)))
        for k in range(lines):
            held = block(index(at_z(lines - k), x, c))
            ss.append(remote(held, held, s_send.at[kind, k], s_recv.at[kind, k], side))
            mine = [held, block(index(at_z(lines - k), 1 - x, c))]
            cs.append([remote(h, h, c_send.at[kind, k, n], c_recv.at[kind, k, n], pair) for n, h in enumerate(mine)])
        return zs, ss, cs

    gx, gr = gather(x_all, 0), gather(r_all, 1)
    order = [0] + sorted(range(1, lines), key=lambda k: (min(k, lines - k), k))
    for (zs, ss, cs), load in ((gx, loads[0]), (gr, loads[1])):
        load.wait()
        for step in order[:0:-1]:
            zs[step - 1].start()
        ss[0].start()
        cs[0][0].start()
    for zs, ss, cs in (gx, gr):
        ss[0].wait_recv()
        cs[0][1].start()
        for k in order[1:]:
            zs[k - 1].wait_recv()
            ss[k].start()
            cs[k][0].start()
        for k in order[1:]:
            ss[k].wait_recv()
            cs[k][1].start()
    for group in gx[2]:
        for copy in group:
            copy.wait_recv()

    loads[2].wait()
    blocks = x_all.shape[0]
    total = jnp.zeros((rows, width), jnp.float32)
    for b in range(blocks):
        f = x_all[b].astype(jnp.float32)
        total = total + f * f
    inv_rms = lax.rsqrt(jnp.sum(total, axis=1, keepdims=True) / (blocks * width) + epsilon)
    for b in range(blocks):
        cols = pl.ds(b * width, width)
        normed[:, cols] = (x_all[b].astype(jnp.float32) * inv_rms * gain[:, cols]).astype(jnp.bfloat16)

    hidden = []
    for e in range(local_count):
        gu_loads[2 * e].wait()
        gu_loads[2 * e + 1].wait()
        acts = jnp.dot(normed[...], wgu[e], preferred_element_type=jnp.float32)
        gate_act, up_act = acts[:, :inner], acts[:, inner:]
        hidden.append((gate_act / (1.0 + jnp.exp(-gate_act)) * up_act).astype(jnp.bfloat16))

    for group in gr[2]:
        for copy in group:
            copy.wait_recv()
    for b in range(blocks):
        rwide[:, pl.ds(b * width, width)] = r_all[b]
    logits = lax.dot_general(
        normed[...], rwide[...], (((1,), (1,)), ((), ())), preferred_element_type=jnp.float32
    )
    loads[3].wait()
    eye = lax.broadcasted_iota(jnp.int32, (rows, rows), 0) == lax.broadcasted_iota(jnp.int32, (rows, rows), 1)
    lane = lax.broadcasted_iota(jnp.int32, logits.shape, 1).astype(jnp.float32)
    picks, chosen = [], []
    for k in range(2):
        row = ids[pl.ds(k, 1), :].astype(jnp.float32)
        pick = jnp.sum(jnp.where(eye, row, 0.0), axis=1, keepdims=True)
        picks.append(pick)
        chosen.append(jnp.sum(jnp.where(lane == pick, logits, 0.0), axis=1, keepdims=True))
    top = jnp.maximum(chosen[0], chosen[1])
    powers = [jnp.exp(v - top) for v in chosen]
    weights = [v / (powers[0] + powers[1]) for v in powers]
    gates = []
    for e in range(local_count):
        number = (y * local_count + e).astype(jnp.float32)
        gates.append(
            jnp.where(picks[0] == number, weights[0], 0.0) + jnp.where(picks[1] == number, weights[1], 0.0)
        )
    down_load.wait()

    def partial(owner):
        cols = pl.ds(pl.multiple_of(owner * width, width), width)
        out = None
        for e in range(local_count):
            term = gates[e] * jnp.dot(hidden[e], wd[e, :, cols], preferred_element_type=jnp.float32)
            out = term if out is None else out + term
        return out

    offsets = [k for k in order[::-1]]
    count = 2 * lines
    pairs = [remote(pair_out.at[m], pair_in.at[m], pair_ss.at[m], pair_rs.at[m], pair) for m in range(count)]
    eps = [remote(ep_out.at[m], ep_in.at[m], ep_ss.at[m], ep_rs.at[m], other) for m in range(count)]
    sides = [remote(side_out.at[j], side_in.at[j], side_ss.at[j], side_rs.at[j], side) for j in range(lines)]
    line = [
        remote(line_out.at[j], line_in.at[j], line_ss.at[j], line_rs.at[j], along(offsets[j])) if offsets[j] else None
        for j in range(lines)
    ]
    mine = pl.ds(pl.multiple_of(y * half, half), half)
    theirs = pl.ds(pl.multiple_of((1 - y) * half, half), half)

    def make(m):
        zz, xx = at_z(offsets[m // 2]), (1 - x if m % 2 == 0 else x)
        pair_out[m] = partial(index(zz, xx, 1 - c))
        pairs[m].start()
        own[m] = partial(index(zz, xx, c))

    def over_ep(m):
        pairs[m].wait_recv()
        ep_out[m] = (own[m, theirs, :] + pair_in[m, theirs, :]).astype(jnp.bfloat16)
        eps[m].start()

    def half_sum(m):
        return own[m, mine, :] + pair_in[m, mine, :] + ep_in[m].astype(jnp.float32)

    def over_side(j):
        eps[2 * j].wait_recv()
        side_out[j] = half_sum(2 * j)
        sides[j].start()

    kept = []

    def over_line(j):
        eps[2 * j + 1].wait_recv()
        sides[j].wait_recv()
        value = half_sum(2 * j + 1) + side_in[j]
        if offsets[j]:
            line_out[j] = value
            line[j].start()
        else:
            kept.append(value)

    for s in range(count + 11):
        if s < count:
            make(s)
        if 0 <= s - 1 < count:
            over_ep(s - 1)
        if s >= 5 and (s - 5) % 2 == 0 and (s - 5) // 2 < lines:
            over_side((s - 5) // 2)
        if s >= 9 and (s - 9) % 2 == 0 and (s - 9) // 2 < lines:
            over_line((s - 9) // 2)
    result = kept[0]
    for j in range(lines):
        if offsets[j]:
            line[j].wait_recv()
            result = result + line_in[j]
    last_out[...] = result.astype(jnp.bfloat16)
    last = remote(last_out, last_in, last_ss.at[0], last_rs.at[0], other)
    last.start()
    o_ref[mine, :] = result.astype(jnp.bfloat16)
    for zs, ss, cs in (gx, gr):
        for copy in zs + ss + [copy for group in cs for copy in group]:
            copy.wait_send()
    for copy in pairs + eps + sides + [copy for copy in line if copy is not None]:
        copy.wait_send()
    last.wait()
    o_ref[theirs, :] = last_in[...]


def fused_shards(lines, activations, norm_gain, router_weight, expert_ids, w_gate, w_up, w_down):
    rows, width = activations.shape
    blocks = 4 * lines
    count = 2 * lines
    local_count, features, inner = w_gate.shape
    experts = router_weight.shape[1]
    half = rows // 2
    f32, bf16 = jnp.float32, jnp.bfloat16
    dma = pltpu.SemaphoreType.DMA
    return pl.pallas_call(
        functools.partial(layer_kernel, lines, local_count),
        out_shape=jax.ShapeDtypeStruct((rows, width), bf16),
        in_specs=[pl.BlockSpec(memory_space=pltpu.HBM)] * 7,
        out_specs=pl.BlockSpec(memory_space=pltpu.VMEM),
        scratch_shapes=[
            pltpu.VMEM((blocks, rows, width), bf16),
            pltpu.VMEM((blocks, experts, width), bf16),
            pltpu.VMEM((1, features), f32),
            pltpu.VMEM(expert_ids.shape[::-1], jnp.int32),
            pltpu.VMEM((local_count, features, 2 * inner), bf16),
            pltpu.VMEM(w_down.shape, bf16),
            pltpu.VMEM((rows, features), bf16),
            pltpu.VMEM((experts, features), bf16),
            pltpu.VMEM((count, rows, width), f32),
            pltpu.VMEM((count, rows, width), f32),
            pltpu.VMEM((count, rows, width), f32),
            pltpu.VMEM((count, half, width), bf16),
            pltpu.VMEM((count, half, width), bf16),
            pltpu.VMEM((lines, half, width), f32),
            pltpu.VMEM((lines, half, width), f32),
            pltpu.VMEM((lines, half, width), f32),
            pltpu.VMEM((lines, half, width), f32),
            pltpu.VMEM((half, width), bf16),
            pltpu.VMEM((half, width), bf16),
            dma((4,)), dma((local_count, 2)), dma((1,)),
            dma((2, lines)), dma((2, lines)), dma((2, lines)), dma((2, lines)),
            dma((2, lines, 2)), dma((2, lines, 2)),
            dma((count,)), dma((count,)), dma((count,)), dma((count,)),
            dma((lines,)), dma((lines,)), dma((lines,)), dma((lines,)), dma((1,)), dma((1,)),
        ],
        compiler_params=pltpu.CompilerParams(
            collective_id=0, has_side_effects=True, vmem_limit_bytes=60 * 1024 * 1024
        ),
    )(activations, norm_gain.astype(f32).reshape(1, -1), router_weight.T, expert_ids.T, w_gate, w_up, w_down)


def summed_rows(portion, rows, axis):
    count = rows * lax.axis_size(axis)
    return lax.psum_scatter(portion(jnp.int32(0), count), axis, scatter_dimension=0, tiled=True)


def shards(activations, norm_gain, router_weight, expert_ids, w_gate, w_up, w_down):
    shard_width = activations.shape[1]
    gathered = lax.all_gather(activations, "tp", axis=1, tiled=True)
    features = gathered.astype(jnp.float32)
    inv_rms = lax.rsqrt(jnp.mean(features * features, axis=1, keepdims=True) + epsilon)
    normed = (features * inv_rms * norm_gain.astype(jnp.float32)).astype(jnp.bfloat16)
    router_full = lax.all_gather(router_weight, "tp", axis=0, tiled=True)
    logits = jnp.dot(normed, router_full, preferred_element_type=jnp.float32)
    expert_total = router_weight.shape[1]
    chosen = jnp.take_along_axis(logits, expert_ids, axis=1)
    weights = jax.nn.softmax(chosen, axis=1)
    gate_dense = jnp.sum(
        weights[:, :, None] * jax.nn.one_hot(expert_ids, expert_total, dtype=jnp.float32), axis=1
    )
    local_count = w_gate.shape[0]
    local_gates = lax.dynamic_slice_in_dim(
        gate_dense, lax.axis_index("ep") * local_count, local_count, 1
    )
    gate_per_expert = local_gates.T
    gate_act = jnp.einsum("td,edf->etf", normed, w_gate, preferred_element_type=jnp.float32)
    up_act = jnp.einsum("td,edf->etf", normed, w_up, preferred_element_type=jnp.float32)
    hidden = (jax.nn.silu(gate_act) * up_act).astype(jnp.bfloat16)

    def weighted_terms(begin_row, row_count):
        columns = lax.dynamic_slice_in_dim(w_down, begin_row, row_count, 2)
        products = jnp.einsum("efc,etf->ect", columns, hidden, preferred_element_type=jnp.float32)
        return jnp.sum(products * gate_per_expert[:, None, :], axis=0)

    own_rows = summed_rows(weighted_terms, shard_width, "tp")
    summed = lax.psum(own_rows, "ep")
    return summed.T.astype(jnp.bfloat16)


def solution(mesh):
    tp = mesh.shape["tp"]
    in_specs = (
        P(None, "tp"),
        P(),
        P("tp", None),
        P(),
        P("ep", None, "tp"),
        P("ep", None, "tp"),
        P("ep", "tp", None),
    )
    out_specs = P(None, "tp")

    def plan(activations, *rest):
        fits = tp % 4 == 0 and mesh.shape["ep"] == 2 and activations.shape[1] % 128 == 0
        fits = fits and activations.shape[0] % 32 == 0 and rest[3].shape[2] % 128 == 0
        part = functools.partial(fused_shards, tp // 4) if fits else shards
        return part(activations, *rest)

    return jax.shard_map(plan, mesh=mesh, in_specs=in_specs, out_specs=out_specs, check_vma=False)
```
